32 devices in a mesh: parts: 2 (over y), shot: 4 (over z), freq: 2 (over x), rep: 2 (over core).
Axes of the slice: x: 2, y: 2, z: 4, core: 2. Of those that a mesh axis runs over, the one named last changes fastest.
Arguments:
- recorded: bfloat16 [2, 4, 2048, 2048], P(None, ('parts', 'freq'), ('shot', 'rep')), parts along dimension 1, may hold values from -6 to 6
- receiver_x: float32 [4096], P('parts'), parts along dimension 0, may hold values from -12800 to 12800
- source_x: float32 [4096], P('parts'), parts along dimension 0, may hold values from -12800 to 12800
Outputs:
- predicted: bfloat16 [2, 4, 2048, 2048], P(None, ('parts', 'freq'), ('shot', 'rep')), parts along dimension 1
The draws below stay inside these ranges and needn't reach their ends.
There are 2 independent parts, one for each index of `parts`. The reference program is written for one: setup_inputs(seed, part) draws one part's arguments, and reference() takes and returns one part's arrays. A program takes and returns all parts, laid end to end along the dimension named above; each array names one. Nothing has to cross between parts.
All inputs are finite; a program needn't handle non-finite values.
Results may differ from the reference program's by a relative error of at most 0.013.
Values may be sent and summed in bfloat16 or wider, within the bound.
A program may use at most 64 MiB of HBM per device.

```python
import math
import jax
import jax.numpy as jnp
from jax import lax

NSRC = 2048
NREC = 2048
NSLOW = 1024
NFREQ = 2


def level_of(stream_key, extent, split, least, high):
    gain, own = 1.0, jax.random.fold_in(stream_key, 6)
    for dim, parts in split:
        heights = jnp.exp(jax.random.uniform(jax.random.fold_in(own, dim), (parts,), jnp.float32, least / len(split), high / len(split)))
        gain = gain * jnp.repeat(heights, extent[dim] // parts).reshape([-1 if axis == dim else 1 for axis in range(len(extent))])
    return gain


def scatter_about(own_key, shape, width, limit, shards=(), kind=jnp.bfloat16):
    values = width * jax.random.normal(own_key, shape, jnp.float32)
    if shards:
        values = values * level_of(own_key, shape, shards, -0.22, 0.18)
    return jnp.clip(values, -limit, limit).astype(kind)


def setup_inputs(seed: int = 0, part: int = 0) -> dict:
    keys = jax.random.split(jax.random.key(seed), 4)
    part_keys = jax.random.split(jax.random.fold_in(keys[3], part), 4)
    return {
        "recorded": scatter_about(part_keys[0], (2, NFREQ, NSRC, NREC), 1.0, 6.0, ((1, 2), (2, 8))),
        "receiver_x": jnp.clip(jax.random.uniform(part_keys[1], (NREC,), jnp.float32, -12800.0, 12800.0), -12800.0, 12800.0),
        "source_x": jnp.clip(jax.random.uniform(part_keys[2], (NSRC,), jnp.float32, -12800.0, 12800.0), -12800.0, 12800.0),
    }


two_pi = 6.283185307179586
base_hertz = 40.0
step_hertz = 0.5
slow_max = 0.0005

def slowness_values(grid_count):
    counts = jnp.arange(grid_count, dtype=jnp.int32)
    return slow_max * ((2 * counts + 1 - grid_count).astype(jnp.float32) / grid_count)

def angle_tables(omegas, positions, slowness_grid):
    phases = (omegas * slowness_grid)[None, :] * positions[:, None]
    return (jnp.cos(phases).astype(jnp.bfloat16), jnp.sin(phases).astype(jnp.bfloat16))

def product(left, right):
    return jnp.dot(left, right, preferred_element_type=jnp.float32)

def reference(recorded, receiver_x, source_x):
    slowness_grid = slowness_values(NSLOW)
    scale_receivers = 1.0 / math.sqrt(NREC)
    scale_sources = 1.0 / math.sqrt(NSRC)
    scale_slices = 1.0 / math.sqrt(NSLOW)

    def one_frequency(inputs):
        index_value, data_real, data_imaginary = inputs
        omegas = two_pi * (base_hertz + step_hertz * index_value)
        receiver_cosine, receiver_sine = angle_tables(omegas, receiver_x, slowness_grid)
        source_cosine, source_sine = angle_tables(omegas, source_x, slowness_grid)
        spread_real = ((product(data_real, receiver_cosine) + product(data_imaginary, receiver_sine)) * scale_receivers).astype(jnp.bfloat16)
        spread_imaginary = ((product(data_imaginary, receiver_cosine) - product(data_real, receiver_sine)) * scale_receivers).astype(jnp.bfloat16)
        plane_real = ((product(source_cosine.T, spread_real) + product(source_sine.T, spread_imaginary)) * scale_sources).astype(jnp.bfloat16)
        plane_imaginary = ((product(source_cosine.T, spread_imaginary) - product(source_sine.T, spread_real)) * scale_sources).astype(jnp.bfloat16)
        multiple_real = ((product(plane_real, plane_real) - product(plane_imaginary, plane_imaginary)) * scale_slices).astype(jnp.bfloat16)
        multiple_imaginary = ((product(plane_real, plane_imaginary) + product(plane_imaginary, plane_real)) * scale_slices).astype(jnp.bfloat16)
        back_real = ((product(source_cosine, multiple_real) - product(source_sine, multiple_imaginary)) * scale_slices).astype(jnp.bfloat16)
        back_imaginary = ((product(source_cosine, multiple_imaginary) + product(source_sine, multiple_real)) * scale_slices).astype(jnp.bfloat16)
        predicted_real = ((product(back_real, receiver_cosine.T) - product(back_imaginary, receiver_sine.T)) * scale_slices).astype(jnp.bfloat16)
        predicted_imaginary = ((product(back_real, receiver_sine.T) + product(back_imaginary, receiver_cosine.T)) * scale_slices).astype(jnp.bfloat16)
        return (predicted_real, predicted_imaginary)
    indices = jnp.arange(NFREQ, dtype=jnp.int32).astype(jnp.float32)
    result_real, result_imaginary = lax.map(one_frequency, (indices, recorded[0], recorded[1]))
    return jnp.stack([result_real, result_imaginary], axis=0)
```

```python
import math

import jax
import jax.numpy as jnp
from jax import lax
from jax.sharding import PartitionSpec as P

NSLOW = 1024

two_pi = 6.283185307179586
base_hertz = 40.0
step_hertz = 0.5
slow_max = 0.0005
GROUP = ("shot", "rep")


def angle_table(omega, positions):
    half = NSLOW // 2
    fine = math.gcd(half, 16)
    unit = (omega * (slow_max / NSLOW)) * positions
    coarse = (jnp.arange(half // fine, dtype=jnp.int32) * (2 * fine)).astype(jnp.float32)[:, None] * unit
    small = (2 * jnp.arange(fine, dtype=jnp.int32) + 1).astype(jnp.float32)[:, None] * unit
    cos_a, sin_a = jnp.cos(coarse)[:, None], jnp.sin(coarse)[:, None]
    cos_b, sin_b = jnp.cos(small)[None], jnp.sin(small)[None]
    cosine = cos_a * cos_b - sin_a * sin_b
    sine = sin_a * cos_b + cos_a * sin_b
    return jnp.stack([cosine, sine]).astype(jnp.bfloat16).reshape(NSLOW, positions.shape[0])


def product(form, left, right):
    return jnp.einsum(form, left, right, preferred_element_type=jnp.float32)


def one_frequency(data, receiver_x, source_x, omega):
    shots = data.shape[1]
    src_count, rec_count = source_x.shape[0], receiver_x.shape[0]
    receiver = angle_table(omega, receiver_x)
    source = angle_table(omega, source_x)
    first = lax.axis_index(GROUP) * shots
    mine = angle_table(omega, lax.dynamic_slice_in_dim(source_x, first, shots, 0))
    spread = (product("csr,jr->csj", data, receiver) * math.sqrt(2.0 / rec_count)).astype(jnp.bfloat16)
    met = lax.all_to_all(spread, GROUP, split_axis=2, concat_axis=1, tiled=True)
    plane = (product("qs,csj->cqj", source, met) * math.sqrt(2.0 / src_count)).astype(jnp.bfloat16)
    planes = lax.all_gather(plane, GROUP, axis=2, tiled=True)
    sign = jnp.where(jnp.arange(NSLOW) < NSLOW // 2, 1.0, -1.0) * math.sqrt(2.0 / NSLOW)
    half_way = (product("qs,cqj->csj", mine, planes) * sign).astype(jnp.bfloat16)
    back_real = product("sm,mj->sj", half_way[0], planes[0]) - product("sm,mj->sj", half_way[1], planes[1])
    back_imaginary = product("sm,mj->sj", half_way[0], planes[1]) + product("sm,mj->sj", half_way[1], planes[0])
    back = (jnp.stack([back_real, back_imaginary]) * math.sqrt(1.0 / NSLOW)).astype(jnp.bfloat16)
    return (product("csj,jr->csr", back, receiver) * math.sqrt(2.0 / NSLOW)).astype(jnp.bfloat16)


def body(recorded, receiver_x, source_x):
    per_device = recorded.shape[1]
    first_freq = lax.axis_index("freq") * per_device
    outs = []
    for k in range(per_device):
        omega = two_pi * (base_hertz + step_hertz * (first_freq + k).astype(jnp.float32))
        outs.append(one_frequency(recorded[:, k], receiver_x, source_x, omega))
    return jnp.stack(outs, axis=1)


def solution(mesh):
    return jax.shard_map(
        body,
        mesh=mesh,
        in_specs=(P(None, ("parts", "freq"), ("shot", "rep"), None), P("parts"), P("parts")),
        out_specs=P(None, ("parts", "freq"), ("shot", "rep"), None),
        check_vma=False,
    )
```

```python
import functools
import math

import jax
import jax.numpy as jnp
from jax import lax
from jax.experimental import pallas as pl
from jax.experimental.pallas import tpu as pltpu
from jax.sharding import PartitionSpec as P

NSLOW = 1024

two_pi = 6.283185307179586
base_hertz = 40.0
step_hertz = 0.5
slow_max = 0.0005
GROUP = ("shot", "rep")


def angle_table(omega, positions):
    half = NSLOW // 2
    fine = math.gcd(half, 16)
    unit = (omega * (slow_max / NSLOW)) * positions
    coarse = (jnp.arange(half // fine, dtype=jnp.int32) * (2 * fine)).astype(jnp.float32)[:, None] * unit
    small = (2 * jnp.arange(fine, dtype=jnp.int32) + 1).astype(jnp.float32)[:, None] * unit
    cos_a, sin_a = jnp.cos(coarse)[:, None], jnp.sin(coarse)[:, None]
    cos_b, sin_b = jnp.cos(small)[None], jnp.sin(small)[None]
    cosine = cos_a * cos_b - sin_a * sin_b
    sine = sin_a * cos_b + cos_a * sin_b
    return jnp.stack([cosine, sine]).astype(jnp.bfloat16).reshape(NSLOW, positions.shape[0])


def product(form, left, right):
    return jnp.einsum(form, left, right, preferred_element_type=jnp.float32)


def one_frequency(data, receiver_x, source_x, omega):
    shots = data.shape[1]
    src_count, rec_count = source_x.shape[0], receiver_x.shape[0]
    receiver = angle_table(omega, receiver_x)
    source = angle_table(omega, source_x)
    first = lax.axis_index(GROUP) * shots
    mine = angle_table(omega, lax.dynamic_slice_in_dim(source_x, first, shots, 0))
    spread = (product("csr,jr->csj", data, receiver) * math.sqrt(2.0 / rec_count)).astype(jnp.bfloat16)
    met = lax.all_to_all(spread, GROUP, split_axis=2, concat_axis=1, tiled=True)
    plane = (product("qs,csj->cqj", source, met) * math.sqrt(2.0 / src_count)).astype(jnp.bfloat16)
    planes = lax.all_gather(plane, GROUP, axis=2, tiled=True)
    sign = jnp.where(jnp.arange(NSLOW) < NSLOW // 2, 1.0, -1.0) * math.sqrt(2.0 / NSLOW)
    half_way = (product("qs,cqj->csj", mine, planes) * sign).astype(jnp.bfloat16)
    back_real = product("sm,mj->sj", half_way[0], planes[0]) - product("sm,mj->sj", half_way[1], planes[1])
    back_imaginary = product("sm,mj->sj", half_way[0], planes[1]) + product("sm,mj->sj", half_way[1], planes[0])
    back = (jnp.stack([back_real, back_imaginary]) * math.sqrt(1.0 / NSLOW)).astype(jnp.bfloat16)
    return (product("csj,jr->csr", back, receiver) * math.sqrt(2.0 / NSLOW)).astype(jnp.bfloat16)


FINE = 16
HALF = NSLOW // 2
COARSE = HALF // FINE
MESH = pl.DeviceIdType.MESH


def angle_factors(omega, positions):
    unit = (omega * (slow_max / NSLOW)) * positions
    steps = jnp.concatenate(
        [jnp.arange(COARSE, dtype=jnp.int32) * (2 * FINE), 2 * jnp.arange(FINE, dtype=jnp.int32) + 1]
    )
    phases = steps.astype(jnp.float32)[:, None] * unit[None, :]
    return jnp.stack([jnp.cos(phases), jnp.sin(phases)])


def fill_table(factors, table):
    count = table.shape[1]
    tile = math.gcd(count, 512)
    for first in range(0, count, tile):
        lanes = slice(first, first + tile)
        cos_b = factors[0, COARSE : COARSE + FINE, lanes]
        sin_b = factors[1, COARSE : COARSE + FINE, lanes]

        def step(a, carry):
            cos_a = factors[0, pl.ds(a, 1), lanes]
            sin_a = factors[1, pl.ds(a, 1), lanes]
            row = pl.multiple_of(a * FINE, FINE)
            table[pl.ds(row, FINE), lanes] = (cos_a * cos_b - sin_a * sin_b).astype(jnp.bfloat16)
            table[pl.ds(HALF + row, FINE), lanes] = (sin_a * cos_b + cos_a * sin_b).astype(jnp.bfloat16)
            return carry

        lax.fori_loop(0, COARSE, step, 0, unroll=4)


def dot(left, right):
    return jnp.dot(left, right, preferred_element_type=jnp.float32)


def whole_kernel(
    chips, data, receiver_f, source_f, out,
    receiver, source, mine, outgoing, met, planes, half_way, back,
    spread_send, spread_recv, plane_send, plane_recv,
):
    cores = 2
    group = chips * cores
    width = NSLOW // group
    shots = data.shape[0] // 2
    z, c = lax.axis_index("shot"), lax.axis_index("rep")
    me = z * cores + c

    def place(d):
        return {"shot": d // cores, "rep": d % cores}

    barrier = pltpu.get_barrier_semaphore()
    for d in range(group):
        @pl.when(d != me)
        def _():
            pl.semaphore_signal(barrier, inc=1, device_id=place(d), device_id_type=MESH)

    fill_table(receiver_f, receiver)
    pl.semaphore_wait(barrier, group - 1)

    def spread_copy(d):
        return pltpu.make_async_remote_copy(
            src_ref=outgoing.at[d], dst_ref=met.at[pl.ds(pl.multiple_of(me * shots, shots), shots)],
            send_sem=spread_send.at[d], recv_sem=spread_recv.at[me], device_id=place(d), device_id_type=MESH,
        )

    scale = math.sqrt(2.0 / data.shape[1])
    order = sorted(range(1, chips), key=lambda k: abs(2 * k - chips)) + [0]
    for offset in order:
        target = lax.rem(z + offset, chips)
        rows = receiver[pl.ds(pl.multiple_of(target * (cores * width), cores * width), cores * width), :]
        part = lax.dot_general(data[...], rows, (((1,), (1,)), ((), ())), preferred_element_type=jnp.float32)
        part = (part * scale).astype(jnp.bfloat16)
        for e in range(cores):
            d = target * cores + e
            real = part[:shots, e * width : (e + 1) * width]
            imaginary = part[shots:, e * width : (e + 1) * width]
            outgoing[d, :, :width] = real
            outgoing[d, :, width:] = imaginary
            if offset == 0:
                @pl.when(d == me)
                def _():
                    own = pl.ds(pl.multiple_of(me * shots, shots), shots)
                    met[own, :width] = real
                    met[own, width:] = imaginary

                @pl.when(d != me)
                def _():
                    spread_copy(d).start()
            else:
                spread_copy(d).start()

    fill_table(source_f, source)
    local = source[:, pl.ds(pl.multiple_of(me * shots, shots), shots)]
    mine[...] = local.T

    for d in range(group):
        @pl.when(d != me)
        def _():
            pltpu.make_async_remote_copy(
                src_ref=outgoing.at[d], dst_ref=met.at[pl.ds(d * shots, shots)],
                send_sem=spread_send.at[d], recv_sem=spread_recv.at[d], device_id=place(d), device_id_type=MESH,
            ).wait_recv()

    scale = math.sqrt(2.0 / source.shape[1])
    tile = 256

    def plane_rows(i, carry):
        rows = pl.ds(pl.multiple_of(i * tile, tile), tile)
        planes[me, rows, :] = (dot(source[rows, :], met[...]) * scale).astype(jnp.bfloat16)
        return carry

    lax.fori_loop(0, NSLOW // tile, plane_rows, 0)

    def plane_copy(way, d):
        to = [{"shot": z + 1, "rep": c}, {"shot": z - 1, "rep": c}, {"shot": z, "rep": 1 - c}][way]
        return pltpu.make_async_remote_copy(
            src_ref=planes.at[d], dst_ref=planes.at[d], send_sem=plane_send.at[way, d], recv_sem=plane_recv.at[d],
            device_id=to, device_id_type=MESH,
        )

    def half_slice(d):
        sign = (1 - 2 * (d // (group // 2))).astype(jnp.float32)
        part = (dot(mine[...], planes[d]) * math.sqrt(2.0 / NSLOW) * sign).astype(jnp.bfloat16)
        lanes = pl.ds(pl.multiple_of(d * width, width), width)
        half_way[:shots, lanes] = part[:, :width]
        half_way[shots:, lanes] = part[:, width:]

    more_up, more_down = z < chips - 1, z > 0

    @pl.when(more_up)
    def _():
        plane_copy(0, me).start()

    @pl.when(more_down)
    def _():
        plane_copy(1, me).start()

    plane_copy(2, me).start()
    half_slice(me)
    for k in range(1, chips):
        for way, sign in ((0, -1), (1, 1)):
            origin = z + sign * k

            @pl.when((origin >= 0) & (origin < chips))
            def _():
                d = origin * cores + c
                plane_copy(2, d).wait_recv()

                @pl.when((more_up, more_down)[way])
                def _():
                    plane_copy(way, d).start()

                plane_copy(2, d).start()
                half_slice(d)

        for sign in ((-1, 1) if k > 1 else (1,)):
            origin = z + sign * (k - 1)

            @pl.when((origin >= 0) & (origin < chips))
            def _():
                d = origin * cores + 1 - c
                plane_copy(2, d).wait_recv()
                half_slice(d)

    for sign in (-1, 1):
        origin = z + sign * (chips - 1)

        @pl.when((origin >= 0) & (origin < chips))
        def _():
            d = origin * cores + 1 - c
            plane_copy(2, d).wait_recv()
            half_slice(d)

    scale_back = math.sqrt(1.0 / NSLOW)

    def back_slice(d, carry):
        both = dot(half_way[...], planes[d])
        lanes = pl.ds(pl.multiple_of(d * width, width), width)
        back[:shots, lanes] = ((both[:shots, :width] - both[shots:, width:]) * scale_back).astype(jnp.bfloat16)
        back[shots:, lanes] = ((both[:shots, width:] + both[shots:, :width]) * scale_back).astype(jnp.bfloat16)
        return carry

    lax.fori_loop(0, group, back_slice, 0)
    scale_out = math.sqrt(2.0 / NSLOW)
    wide = math.gcd(out.shape[1], 512)

    def out_columns(i, carry):
        lanes = pl.ds(pl.multiple_of(i * wide, wide), wide)
        out[:, lanes] = (dot(back[...], receiver[:, lanes]) * scale_out).astype(jnp.bfloat16)
        return carry

    lax.fori_loop(0, out.shape[1] // wide, out_columns, 0)

    for d in range(group):
        @pl.when(d != me)
        def _():
            spread_copy(d).wait_send()
    plane_copy(2, me).wait_send()

    @pl.when(more_up)
    def _():
        plane_copy(0, me).wait_send()

    @pl.when(more_down)
    def _():
        plane_copy(1, me).wait_send()

    for k in range(1, chips):
        for way, sign in ((0, -1), (1, 1)):
            origin = z + sign * k

            @pl.when((origin >= 0) & (origin < chips))
            def _():
                d = origin * cores + c

                @pl.when((more_up, more_down)[way])
                def _():
                    plane_copy(way, d).wait_send()

                plane_copy(2, d).wait_send()


def one_frequency_fused(chips, data, receiver_x, source_x, omega):
    shots, rec_count = data.shape[1:]
    src_count = source_x.shape[0]
    group = 2 * chips
    width = NSLOW // group
    vmem = pl.BlockSpec(memory_space=pltpu.VMEM)
    half = jnp.bfloat16
    result = pl.pallas_call(
        functools.partial(whole_kernel, chips),
        out_shape=jax.ShapeDtypeStruct((2 * shots, rec_count), half),
        in_specs=[vmem] * 3,
        out_specs=vmem,
        scratch_shapes=[
            pltpu.VMEM((NSLOW, rec_count), half),
            pltpu.VMEM((NSLOW, src_count), half),
            pltpu.VMEM((shots, NSLOW), half),
            pltpu.VMEM((group, shots, 2 * width), half),
            pltpu.VMEM((src_count, 2 * width), half),
            pltpu.VMEM((group, NSLOW, 2 * width), half),
            pltpu.VMEM((2 * shots, NSLOW), half),
            pltpu.VMEM((2 * shots, NSLOW), half),
            pltpu.SemaphoreType.DMA((group,)),
            pltpu.SemaphoreType.DMA((group,)),
            pltpu.SemaphoreType.DMA((3, group)),
            pltpu.SemaphoreType.DMA((group,)),
        ],
        compiler_params=pltpu.CompilerParams(
            collective_id=0, has_side_effects=True, vmem_limit_bytes=60 * 1024 * 1024
        ),
        name="plane_wave_multiples",
    )(data.reshape(2 * shots, rec_count), angle_factors(omega, receiver_x), angle_factors(omega, source_x))
    return result.reshape(2, shots, rec_count)


def fits(mesh_shape, shots):
    group = mesh_shape["shot"] * mesh_shape["rep"]
    return mesh_shape["rep"] == 2 and NSLOW % (128 * group) == 0 and shots % 128 == 0


def body(chips, fused, recorded, receiver_x, source_x):
    per_device = recorded.shape[1]
    first_freq = lax.axis_index("freq") * per_device
    outs = []
    for k in range(per_device):
        omega = two_pi * (base_hertz + step_hertz * (first_freq + k).astype(jnp.float32))
        if fused(recorded.shape[2]):
            outs.append(one_frequency_fused(chips, recorded[:, k], receiver_x, source_x, omega))
        else:
            outs.append(one_frequency(recorded[:, k], receiver_x, source_x, omega))
    return jnp.stack(outs, axis=1)


def solution(mesh):
    return jax.shard_map(
        functools.partial(body, mesh.shape["shot"], functools.partial(fits, mesh.shape)),
        mesh=mesh,
        in_specs=(P(None, ("parts", "freq"), ("shot", "rep"), None), P("parts"), P("parts")),
        out_specs=P(None, ("parts", "freq"), ("shot", "rep"), None),
        check_vma=False,
    )
```

```python
import functools
import math

import jax
import jax.numpy as jnp
from jax import lax
from jax.experimental import pallas as pl
from jax.experimental.pallas import tpu as pltpu
from jax.sharding import PartitionSpec as P

NSLOW = 1024

two_pi = 6.283185307179586
base_hertz = 40.0
step_hertz = 0.5
slow_max = 0.0005
GROUP = ("shot", "rep")


def angle_table(omega, positions):
    half = NSLOW // 2
    fine = math.gcd(half, 16)
    unit = (omega * (slow_max / NSLOW)) * positions
    coarse = (jnp.arange(half // fine, dtype=jnp.int32) * (2 * fine)).astype(jnp.float32)[:, None] * unit
    small = (2 * jnp.arange(fine, dtype=jnp.int32) + 1).astype(jnp.float32)[:, None] * unit
    cos_a, sin_a = jnp.cos(coarse)[:, None], jnp.sin(coarse)[:, None]
    cos_b, sin_b = jnp.cos(small)[None], jnp.sin(small)[None]
    cosine = cos_a * cos_b - sin_a * sin_b
    sine = sin_a * cos_b + cos_a * sin_b
    return jnp.stack([cosine, sine]).astype(jnp.bfloat16).reshape(NSLOW, positions.shape[0])


def product(form, left, right):
    return jnp.einsum(form, left, right, preferred_element_type=jnp.float32)


def one_frequency(data, receiver_x, source_x, omega):
    shots = data.shape[1]
    src_count, rec_count = source_x.shape[0], receiver_x.shape[0]
    receiver = angle_table(omega, receiver_x)
    source = angle_table(omega, source_x)
    first = lax.axis_index(GROUP) * shots
    mine = angle_table(omega, lax.dynamic_slice_in_dim(source_x, first, shots, 0))
    spread = (product("csr,jr->csj", data, receiver) * math.sqrt(2.0 / rec_count)).astype(jnp.bfloat16)
    met = lax.all_to_all(spread, GROUP, split_axis=2, concat_axis=1, tiled=True)
    plane = (product("qs,csj->cqj", source, met) * math.sqrt(2.0 / src_count)).astype(jnp.bfloat16)
    planes = lax.all_gather(plane, GROUP, axis=2, tiled=True)
    sign = jnp.where(jnp.arange(NSLOW) < NSLOW // 2, 1.0, -1.0) * math.sqrt(2.0 / NSLOW)
    half_way = (product("qs,cqj->csj", mine, planes) * sign).astype(jnp.bfloat16)
    back_real = product("sm,mj->sj", half_way[0], planes[0]) - product("sm,mj->sj", half_way[1], planes[1])
    back_imaginary = product("sm,mj->sj", half_way[0], planes[1]) + product("sm,mj->sj", half_way[1], planes[0])
    back = (jnp.stack([back_real, back_imaginary]) * math.sqrt(1.0 / NSLOW)).astype(jnp.bfloat16)
    return (product("csj,jr->csr", back, receiver) * math.sqrt(2.0 / NSLOW)).astype(jnp.bfloat16)


FINE = 16
HALF = NSLOW // 2
COARSE = HALF // FINE
MESH = pl.DeviceIdType.MESH


def fill_factors(omega, positions, factors):
    count = positions.shape[1]
    tile = math.gcd(count, 256)
    sines = [(-1.0) ** n / math.factorial(2 * n + 1) for n in range(7)]
    cosines = [(-1.0) ** n / math.factorial(2 * n) for n in range(8)]
    turn_high = 6.28125
    turn_low = two_pi - turn_high

    def step(i, carry):
        lanes = pl.ds(pl.multiple_of(i * tile, tile), tile)
        unit = positions[:, lanes] * (omega * (slow_max / NSLOW))
        row = lax.broadcasted_iota(jnp.int32, (COARSE + FINE, tile), 0)
        steps = jnp.where(row < COARSE, row * (2 * FINE), 2 * (row - COARSE) + 1).astype(jnp.float32)
        phase = steps * unit
        turns = jnp.floor(phase * (1.0 / two_pi) + 0.5)
        half = 0.5 * ((phase - turns * turn_high) - turns * turn_low)
        square = half * half
        sine, cosine = sines[-1], cosines[-1]
        for term in reversed(sines[:-1]):
            sine = sine * square + term
        for term in reversed(cosines[:-1]):
            cosine = cosine * square + term
        sine = sine * half
        factors[0, :, lanes] = 1.0 - 2.0 * sine * sine
        factors[1, :, lanes] = 2.0 * sine * cosine
        return carry

    lax.fori_loop(0, count // tile, step, 0)


def fill_table(factors, table):
    count = table.shape[1]
    tile = math.gcd(count, 512)
    for first in range(0, count, tile):
        lanes = slice(first, first + tile)
        cos_b = factors[0, COARSE : COARSE + FINE, lanes]
        sin_b = factors[1, COARSE : COARSE + FINE, lanes]

        def step(a, carry):
            cos_a = factors[0, pl.ds(a, 1), lanes]
            sin_a = factors[1, pl.ds(a, 1), lanes]
            row = pl.multiple_of(a * FINE, FINE)
            table[pl.ds(row, FINE), lanes] = (cos_a * cos_b - sin_a * sin_b).astype(jnp.bfloat16)
            table[pl.ds(HALF + row, FINE), lanes] = (sin_a * cos_b + cos_a * sin_b).astype(jnp.bfloat16)
            return carry

        lax.fori_loop(0, COARSE, step, 0, unroll=4)


def dot(left, right):
    return jnp.dot(left, right, preferred_element_type=jnp.float32)


def whole_kernel(
    chips, first_hertz, data, receiver_x, source_x, out,
    receiver, source, receiver_f, source_f, mine, outgoing, met, planes, half_way, back,
    spread_send, spread_recv, plane_send, plane_recv,
):
    cores = 2
    group = chips * cores
    width = NSLOW // group
    shots = data.shape[0] // 2
    z, c = lax.axis_index("shot"), lax.axis_index("rep")
    me = z * cores + c

    def place(d):
        return {"shot": d // cores, "rep": d % cores}

    barrier = pltpu.get_barrier_semaphore()
    for d in range(group):
        @pl.when(d != me)
        def _():
            pl.semaphore_signal(barrier, inc=1, device_id=place(d), device_id_type=MESH)

    hertz = first_hertz(lax.axis_index("freq")).astype(jnp.float32)
    omega = two_pi * (base_hertz + step_hertz * hertz)
    fill_factors(omega, receiver_x, receiver_f)
    fill_table(receiver_f, receiver)
    pl.semaphore_wait(barrier, group - 1)

    def spread_copy(h, d):
        return pltpu.make_async_remote_copy(
            src_ref=outgoing.at[h, d], dst_ref=met.at[h, pl.ds(pl.multiple_of(me * shots, shots), shots)],
            send_sem=spread_send.at[h, d], recv_sem=spread_recv.at[h, me],
            device_id=place(d), device_id_type=MESH,
        )

    scale = math.sqrt(2.0 / data.shape[1])
    order = sorted(range(1, chips), key=lambda k: abs(2 * k - chips)) + [0]
    for h in range(2):
        for offset in order:
            target = lax.rem(z + offset, chips)
            rows = receiver[pl.ds(pl.multiple_of(target * (cores * width), cores * width), cores * width), :]
            part = lax.dot_general(
                data[h * shots : (h + 1) * shots, :], rows, (((1,), (1,)), ((), ())),
                preferred_element_type=jnp.float32,
            )
            part = (part * scale).astype(jnp.bfloat16)
            for e in range(cores):
                d = target * cores + e
                piece = part[:, e * width : (e + 1) * width]
                if offset == 0:
                    @pl.when(d == me)
                    def _():
                        met[h, pl.ds(pl.multiple_of(me * shots, shots), shots), :] = piece

                    @pl.when(d != me)
                    def _():
                        outgoing[h, d] = piece
                        spread_copy(h, d).start()
                else:
                    outgoing[h, d] = piece
                    spread_copy(h, d).start()

    fill_factors(omega, source_x, source_f)
    fill_table(source_f, source)
    local = source[:, pl.ds(pl.multiple_of(me * shots, shots), shots)]
    mine[...] = local.T

    def plane_copy(way, h, d):
        to = [{"shot": z + 1, "rep": c}, {"shot": z - 1, "rep": c}, {"shot": z, "rep": 1 - c}][way]
        piece = planes.at[d, :, h * width : (h + 1) * width]
        return pltpu.make_async_remote_copy(
            src_ref=piece, dst_ref=piece, send_sem=plane_send.at[way, h, d], recv_sem=plane_recv.at[h, d],
            device_id=to, device_id_type=MESH,
        )

    scale = math.sqrt(2.0 / source.shape[1])
    tile = 256
    more_up, more_down = z < chips - 1, z > 0
    for h in range(2):
        for d in range(group):
            @pl.when(d != me)
            def _():
                pltpu.make_async_remote_copy(
                    src_ref=outgoing.at[h, d], dst_ref=met.at[h, pl.ds(d * shots, shots)],
                    send_sem=spread_send.at[h, d], recv_sem=spread_recv.at[h, d],
                    device_id=place(d), device_id_type=MESH,
                ).wait_recv()

        def plane_rows(i, carry):
            rows = pl.ds(pl.multiple_of(i * tile, tile), tile)
            piece = (dot(source[rows, :], met[h]) * scale).astype(jnp.bfloat16)
            planes[me, rows, h * width : (h + 1) * width] = piece
            return carry

        lax.fori_loop(0, NSLOW // tile, plane_rows, 0)

        @pl.when(more_up)
        def _():
            plane_copy(0, h, me).start()

        @pl.when(more_down)
        def _():
            plane_copy(1, h, me).start()

        plane_copy(2, h, me).start()

    def half_slice(d):
        sign = (1 - 2 * (d // (group // 2))).astype(jnp.float32)
        part = (dot(mine[...], planes[d]) * math.sqrt(2.0 / NSLOW) * sign).astype(jnp.bfloat16)
        lanes = pl.ds(pl.multiple_of(d * width, width), width)
        half_way[:shots, lanes] = part[:, :width]
        half_way[shots:, lanes] = part[:, width:]

    half_slice(me)
    for k in range(1, chips):
        for h in range(2):
            for way, sign in ((0, -1), (1, 1)):
                origin = z + sign * k

                @pl.when((origin >= 0) & (origin < chips))
                def _():
                    d = origin * cores + c
                    plane_copy(2, h, d).wait_recv()

                    @pl.when((more_up, more_down)[way])
                    def _():
                        plane_copy(way, h, d).start()

                    plane_copy(2, h, d).start()
                    if h == 1:
                        half_slice(d)

        for sign in ((-1, 1) if k > 1 else (1,)):
            origin = z + sign * (k - 1)

            @pl.when((origin >= 0) & (origin < chips))
            def _():
                d = origin * cores + 1 - c
                plane_copy(2, 0, d).wait_recv()
                plane_copy(2, 1, d).wait_recv()
                half_slice(d)

    for sign in (-1, 1):
        origin = z + sign * (chips - 1)

        @pl.when((origin >= 0) & (origin < chips))
        def _():
            d = origin * cores + 1 - c
            plane_copy(2, 0, d).wait_recv()
            plane_copy(2, 1, d).wait_recv()
            half_slice(d)

    scale_back = math.sqrt(1.0 / NSLOW)

    def back_slice(d, carry):
        both = dot(half_way[...], planes[d])
        lanes = pl.ds(pl.multiple_of(d * width, width), width)
        back[:shots, lanes] = ((both[:shots, :width] - both[shots:, width:]) * scale_back).astype(jnp.bfloat16)
        back[shots:, lanes] = ((both[:shots, width:] + both[shots:, :width]) * scale_back).astype(jnp.bfloat16)
        return carry

    lax.fori_loop(0, group, back_slice, 0)
    scale_out = math.sqrt(2.0 / NSLOW)
    wide = math.gcd(out.shape[1], 512)

    def out_columns(i, carry):
        lanes = pl.ds(pl.multiple_of(i * wide, wide), wide)
        out[:, lanes] = (dot(back[...], receiver[:, lanes]) * scale_out).astype(jnp.bfloat16)
        return carry

    lax.fori_loop(0, out.shape[1] // wide, out_columns, 0)

    for h in range(2):
        for d in range(group):
            @pl.when(d != me)
            def _():
                spread_copy(h, d).wait_send()
        plane_copy(2, h, me).wait_send()

        @pl.when(more_up)
        def _():
            plane_copy(0, h, me).wait_send()

        @pl.when(more_down)
        def _():
            plane_copy(1, h, me).wait_send()

        for k in range(1, chips):
            for way, sign in ((0, -1), (1, 1)):
                origin = z + sign * k

                @pl.when((origin >= 0) & (origin < chips))
                def _():
                    d = origin * cores + c

                    @pl.when((more_up, more_down)[way])
                    def _():
                        plane_copy(way, h, d).wait_send()

                    plane_copy(2, h, d).wait_send()


def one_frequency_fused(chips, first_hertz, data, receiver_x, source_x):
    shots, rec_count = data.shape[1:]
    src_count = source_x.shape[0]
    group = 2 * chips
    width = NSLOW // group
    vmem = pl.BlockSpec(memory_space=pltpu.VMEM)
    half = jnp.bfloat16
    result = pl.pallas_call(
        functools.partial(whole_kernel, chips, first_hertz),
        out_shape=jax.ShapeDtypeStruct((2 * shots, rec_count), half),
        in_specs=[vmem] * 3,
        out_specs=vmem,
        scratch_shapes=[
            pltpu.VMEM((NSLOW, rec_count), half),
            pltpu.VMEM((NSLOW, src_count), half),
            pltpu.VMEM((2, COARSE + FINE, rec_count), jnp.float32),
            pltpu.VMEM((2, COARSE + FINE, src_count), jnp.float32),
            pltpu.VMEM((shots, NSLOW), half),
            pltpu.VMEM((2, group, shots, width), half),
            pltpu.VMEM((2, src_count, width), half),
            pltpu.VMEM((group, NSLOW, 2 * width), half),
            pltpu.VMEM((2 * shots, NSLOW), half),
            pltpu.VMEM((2 * shots, NSLOW), half),
            pltpu.SemaphoreType.DMA((2, group)),
            pltpu.SemaphoreType.DMA((2, group)),
            pltpu.SemaphoreType.DMA((3, 2, group)),
            pltpu.SemaphoreType.DMA((2, group)),
        ],
        compiler_params=pltpu.CompilerParams(
            collective_id=0, has_side_effects=True, vmem_limit_bytes=60 * 1024 * 1024
        ),
        name="plane_wave_multiples",
    )(data.reshape(2 * shots, rec_count), receiver_x.reshape(1, rec_count), source_x.reshape(1, src_count))
    return result.reshape(2, shots, rec_count)


def fits(mesh_shape, shots):
    group = mesh_shape["shot"] * mesh_shape["rep"]
    return mesh_shape["rep"] == 2 and NSLOW % (128 * group) == 0 and shots % 128 == 0


def body(chips, fused, recorded, receiver_x, source_x):
    per_device = recorded.shape[1]
    first_freq = lax.axis_index("freq") * per_device
    outs = []
    for k in range(per_device):
        omega = two_pi * (base_hertz + step_hertz * (first_freq + k).astype(jnp.float32))
        if fused(recorded.shape[2]):
            first_hertz = functools.partial(lambda k, f: f * per_device + k, k)
            outs.append(one_frequency_fused(chips, first_hertz, recorded[:, k], receiver_x, source_x))
        else:
            outs.append(one_frequency(recorded[:, k], receiver_x, source_x, omega))
    return jnp.stack(outs, axis=1)


def solution(mesh):
    return jax.shard_map(
        functools.partial(body, mesh.shape["shot"], functools.partial(fits, mesh.shape)),
        mesh=mesh,
        in_specs=(P(None, ("parts", "freq"), ("shot", "rep"), None), P("parts"), P("parts")),
        out_specs=P(None, ("parts", "freq"), ("shot", "rep"), None),
        check_vma=False,
    )
```

```python
import functools
import math

import jax
import jax.numpy as jnp
from jax import lax
from jax.experimental import pallas as pl
from jax.experimental.pallas import tpu as pltpu
from jax.sharding import PartitionSpec as P

NSLOW = 1024

two_pi = 6.283185307179586
base_hertz = 40.0
step_hertz = 0.5
slow_max = 0.0005
GROUP = ("shot", "rep")


def angle_table(omega, positions):
    half = NSLOW // 2
    fine = math.gcd(half, 16)
    unit = (omega * (slow_max / NSLOW)) * positions
    coarse = (jnp.arange(half // fine, dtype=jnp.int32) * (2 * fine)).astype(jnp.float32)[:, None] * unit
    small = (2 * jnp.arange(fine, dtype=jnp.int32) + 1).astype(jnp.float32)[:, None] * unit
    cos_a, sin_a = jnp.cos(coarse)[:, None], jnp.sin(coarse)[:, None]
    cos_b, sin_b = jnp.cos(small)[None], jnp.sin(small)[None]
    cosine = cos_a * cos_b - sin_a * sin_b
    sine = sin_a * cos_b + cos_a * sin_b
    return jnp.stack([cosine, sine]).astype(jnp.bfloat16).reshape(NSLOW, positions.shape[0])


def product(form, left, right):
    return jnp.einsum(form, left, right, preferred_element_type=jnp.float32)


def one_frequency(data, receiver_x, source_x, omega):
    shots = data.shape[1]
    src_count, rec_count = source_x.shape[0], receiver_x.shape[0]
    receiver = angle_table(omega, receiver_x)
    source = angle_table(omega, source_x)
    first = lax.axis_index(GROUP) * shots
    mine = angle_table(omega, lax.dynamic_slice_in_dim(source_x, first, shots, 0))
    spread = (product("csr,jr->csj", data, receiver) * math.sqrt(2.0 / rec_count)).astype(jnp.bfloat16)
    met = lax.all_to_all(spread, GROUP, split_axis=2, concat_axis=1, tiled=True)
    plane = (product("qs,csj->cqj", source, met) * math.sqrt(2.0 / src_count)).astype(jnp.bfloat16)
    planes = lax.all_gather(plane, GROUP, axis=2, tiled=True)
    sign = jnp.where(jnp.arange(NSLOW) < NSLOW // 2, 1.0, -1.0) * math.sqrt(2.0 / NSLOW)
    half_way = (product("qs,cqj->csj", mine, planes) * sign).astype(jnp.bfloat16)
    back_real = product("sm,mj->sj", half_way[0], planes[0]) - product("sm,mj->sj", half_way[1], planes[1])
    back_imaginary = product("sm,mj->sj", half_way[0], planes[1]) + product("sm,mj->sj", half_way[1], planes[0])
    back = (jnp.stack([back_real, back_imaginary]) * math.sqrt(1.0 / NSLOW)).astype(jnp.bfloat16)
    return (product("csj,jr->csr", back, receiver) * math.sqrt(2.0 / NSLOW)).astype(jnp.bfloat16)


FINE = 16
HALF = NSLOW // 2
COARSE = HALF // FINE
MESH = pl.DeviceIdType.MESH


def fill_factors(omega, positions, factors):
    count = positions.shape[1]
    tile = math.gcd(count, 256)
    sines = [(-1.0) ** n / math.factorial(2 * n + 1) for n in range(7)]
    cosines = [(-1.0) ** n / math.factorial(2 * n) for n in range(8)]
    turn_high = 6.28125
    turn_low = two_pi - turn_high

    def step(i, carry):
        lanes = pl.ds(pl.multiple_of(i * tile, tile), tile)
        unit = positions[:, lanes] * (omega * (slow_max / NSLOW))
        row = lax.broadcasted_iota(jnp.int32, (COARSE + FINE, tile), 0)
        steps = jnp.where(row < COARSE, row * (2 * FINE), 2 * (row - COARSE) + 1).astype(jnp.float32)
        phase = steps * unit
        turns = jnp.floor(phase * (1.0 / two_pi) + 0.5)
        half = 0.5 * ((phase - turns * turn_high) - turns * turn_low)
        square = half * half
        sine, cosine = sines[-1], cosines[-1]
        for term in reversed(sines[:-1]):
            sine = sine * square + term
        for term in reversed(cosines[:-1]):
            cosine = cosine * square + term
        sine = sine * half
        factors[0, :, lanes] = 1.0 - 2.0 * sine * sine
        factors[1, :, lanes] = 2.0 * sine * cosine
        return carry

    lax.fori_loop(0, count // tile, step, 0)


def fill_table(factors, table):
    count = table.shape[1]
    tile = math.gcd(count, 512)
    for first in range(0, count, tile):
        lanes = slice(first, first + tile)
        cos_b = factors[0, COARSE : COARSE + FINE, lanes]
        sin_b = factors[1, COARSE : COARSE + FINE, lanes]

        def step(a, carry):
            cos_a = factors[0, pl.ds(a, 1), lanes]
            sin_a = factors[1, pl.ds(a, 1), lanes]
            row = pl.multiple_of(a * FINE, FINE)
            table[pl.ds(row, FINE), lanes] = (cos_a * cos_b - sin_a * sin_b).astype(jnp.bfloat16)
            table[pl.ds(HALF + row, FINE), lanes] = (sin_a * cos_b + cos_a * sin_b).astype(jnp.bfloat16)
            return carry

        lax.fori_loop(0, COARSE, step, 0, unroll=4)


def dot(left, right):
    return jnp.dot(left, right, preferred_element_type=jnp.float32)


def whole_kernel(
    chips, first_hertz, data, receiver_x, source_x, back, kept,
    receiver, source, receiver_f, source_f, mine, outgoing, met, planes, half_way,
    spread_send, spread_recv, plane_send, plane_recv, kept_sem,
):
    cores = 2
    group = chips * cores
    width = NSLOW // group
    shots = data.shape[0] // 2
    z, c = lax.axis_index("shot"), lax.axis_index("rep")
    me = z * cores + c

    def place(d):
        return {"shot": d // cores, "rep": d % cores}

    barrier = pltpu.get_barrier_semaphore()
    for d in range(group):
        @pl.when(d != me)
        def _():
            pl.semaphore_signal(barrier, inc=1, device_id=place(d), device_id_type=MESH)

    hertz = first_hertz(lax.axis_index("freq")).astype(jnp.float32)
    omega = two_pi * (base_hertz + step_hertz * hertz)
    fill_factors(omega, receiver_x, receiver_f)
    fill_table(receiver_f, receiver)
    pl.semaphore_wait(barrier, group - 1)

    def spread_copy(h, d):
        return pltpu.make_async_remote_copy(
            src_ref=outgoing.at[h, d], dst_ref=met.at[h, pl.ds(pl.multiple_of(me * shots, shots), shots)],
            send_sem=spread_send.at[h, d], recv_sem=spread_recv.at[h, me],
            device_id=place(d), device_id_type=MESH,
        )

    scale = math.sqrt(2.0 / data.shape[1])
    order = sorted(range(1, chips), key=lambda k: abs(2 * k - chips)) + [0]
    for h in range(2):
        for offset in order:
            target = lax.rem(z + offset, chips)
            rows = receiver[pl.ds(pl.multiple_of(target * (cores * width), cores * width), cores * width), :]
            part = lax.dot_general(
                data[h * shots : (h + 1) * shots, :], rows, (((1,), (1,)), ((), ())),
                preferred_element_type=jnp.float32,
            )
            part = (part * scale).astype(jnp.bfloat16)
            for e in range(cores):
                d = target * cores + e
                piece = part[:, e * width : (e + 1) * width]
                if offset == 0:
                    @pl.when(d == me)
                    def _():
                        met[h, pl.ds(pl.multiple_of(me * shots, shots), shots), :] = piece

                    @pl.when(d != me)
                    def _():
                        outgoing[h, d] = piece
                        spread_copy(h, d).start()
                else:
                    outgoing[h, d] = piece
                    spread_copy(h, d).start()

    keep = pltpu.make_async_copy(receiver, kept, kept_sem)
    keep.start()

    fill_factors(omega, source_x, source_f)
    fill_table(source_f, source)
    local = source[:, pl.ds(pl.multiple_of(me * shots, shots), shots)]
    mine[...] = local.T

    def plane_copy(way, h, d):
        to = [{"shot": z + 1, "rep": c}, {"shot": z - 1, "rep": c}, {"shot": z, "rep": 1 - c}][way]
        piece = planes.at[d, :, h * width : (h + 1) * width]
        return pltpu.make_async_remote_copy(
            src_ref=piece, dst_ref=piece, send_sem=plane_send.at[way, h, d], recv_sem=plane_recv.at[h, d],
            device_id=to, device_id_type=MESH,
        )

    scale = math.sqrt(2.0 / source.shape[1])
    tile = 256
    more_up, more_down = z < chips - 1, z > 0
    for h in range(2):
        for d in range(group):
            @pl.when(d != me)
            def _():
                pltpu.make_async_remote_copy(
                    src_ref=outgoing.at[h, d], dst_ref=met.at[h, pl.ds(d * shots, shots)],
                    send_sem=spread_send.at[h, d], recv_sem=spread_recv.at[h, d],
                    device_id=place(d), device_id_type=MESH,
                ).wait_recv()

        def plane_rows(i, carry):
            rows = pl.ds(pl.multiple_of(i * tile, tile), tile)
            piece = (dot(source[rows, :], met[h]) * scale).astype(jnp.bfloat16)
            planes[me, rows, h * width : (h + 1) * width] = piece
            return carry

        lax.fori_loop(0, NSLOW // tile, plane_rows, 0)

        @pl.when(more_up)
        def _():
            plane_copy(0, h, me).start()

        @pl.when(more_down)
        def _():
            plane_copy(1, h, me).start()

        plane_copy(2, h, me).start()

    def half_slice(d):
        sign = (1 - 2 * (d // (group // 2))).astype(jnp.float32)
        part = (dot(mine[...], planes[d]) * math.sqrt(2.0 / NSLOW) * sign).astype(jnp.bfloat16)
        lanes = pl.ds(pl.multiple_of(d * width, width), width)
        half_way[:shots, lanes] = part[:, :width]
        half_way[shots:, lanes] = part[:, width:]

    half_slice(me)
    for k in range(1, chips):
        for h in range(2):
            for way, sign in ((0, -1), (1, 1)):
                origin = z + sign * k

                @pl.when((origin >= 0) & (origin < chips))
                def _():
                    d = origin * cores + c
                    plane_copy(2, h, d).wait_recv()

                    @pl.when((more_up, more_down)[way])
                    def _():
                        plane_copy(way, h, d).start()

                    plane_copy(2, h, d).start()
                    if h == 1:
                        half_slice(d)

        for sign in ((-1, 1) if k > 1 else (1,)):
            origin = z + sign * (k - 1)

            @pl.when((origin >= 0) & (origin < chips))
            def _():
                d = origin * cores + 1 - c
                plane_copy(2, 0, d).wait_recv()
                plane_copy(2, 1, d).wait_recv()
                half_slice(d)

    for sign in (-1, 1):
        origin = z + sign * (chips - 1)

        @pl.when((origin >= 0) & (origin < chips))
        def _():
            d = origin * cores + 1 - c
            plane_copy(2, 0, d).wait_recv()
            plane_copy(2, 1, d).wait_recv()
            half_slice(d)

    scale_back = math.sqrt(1.0 / NSLOW)

    def back_slice(d, carry):
        both = dot(half_way[...], planes[d])
        lanes = pl.ds(pl.multiple_of(d * width, width), width)
        back[:shots, lanes] = ((both[:shots, :width] - both[shots:, width:]) * scale_back).astype(jnp.bfloat16)
        back[shots:, lanes] = ((both[:shots, width:] + both[shots:, :width]) * scale_back).astype(jnp.bfloat16)
        return carry

    lax.fori_loop(0, group, back_slice, 0)
    keep.wait()
    for h in range(2):
        for d in range(group):
            @pl.when(d != me)
            def _():
                spread_copy(h, d).wait_send()
        plane_copy(2, h, me).wait_send()

        @pl.when(more_up)
        def _():
            plane_copy(0, h, me).wait_send()

        @pl.when(more_down)
        def _():
            plane_copy(1, h, me).wait_send()

        for k in range(1, chips):
            for way, sign in ((0, -1), (1, 1)):
                origin = z + sign * k

                @pl.when((origin >= 0) & (origin < chips))
                def _():
                    d = origin * cores + c

                    @pl.when((more_up, more_down)[way])
                    def _():
                        plane_copy(way, h, d).wait_send()

                    plane_copy(2, h, d).wait_send()


def one_frequency_fused(chips, first_hertz, data, receiver_x, source_x):
    shots, rec_count = data.shape[1:]
    src_count = source_x.shape[0]
    group = 2 * chips
    width = NSLOW // group
    vmem = pl.BlockSpec(memory_space=pltpu.VMEM)
    half = jnp.bfloat16
    back, receiver = pl.pallas_call(
        functools.partial(whole_kernel, chips, first_hertz),
        out_shape=(
            jax.ShapeDtypeStruct((2 * shots, NSLOW), half),
            jax.ShapeDtypeStruct((NSLOW, rec_count), half),
        ),
        in_specs=[vmem] * 3,
        out_specs=(vmem, pl.BlockSpec(memory_space=pl.ANY)),
        scratch_shapes=[
            pltpu.VMEM((NSLOW, rec_count), half),
            pltpu.VMEM((NSLOW, src_count), half),
            pltpu.VMEM((2, COARSE + FINE, rec_count), jnp.float32),
            pltpu.VMEM((2, COARSE + FINE, src_count), jnp.float32),
            pltpu.VMEM((shots, NSLOW), half),
            pltpu.VMEM((2, group, shots, width), half),
            pltpu.VMEM((2, src_count, width), half),
            pltpu.VMEM((group, NSLOW, 2 * width), half),
            pltpu.VMEM((2 * shots, NSLOW), half),
            pltpu.SemaphoreType.DMA((2, group)),
            pltpu.SemaphoreType.DMA((2, group)),
            pltpu.SemaphoreType.DMA((3, 2, group)),
            pltpu.SemaphoreType.DMA((2, group)),
            pltpu.SemaphoreType.DMA,
        ],
        compiler_params=pltpu.CompilerParams(
            collective_id=0, has_side_effects=True, vmem_limit_bytes=60 * 1024 * 1024
        ),
        name="plane_wave_multiples",
    )(data.reshape(2 * shots, rec_count), receiver_x.reshape(1, rec_count), source_x.reshape(1, src_count))
    result = (dot(back, receiver) * math.sqrt(2.0 / NSLOW)).astype(half)
    return result.reshape(2, shots, rec_count)


def fits(mesh_shape, shots):
    group = mesh_shape["shot"] * mesh_shape["rep"]
    return mesh_shape["rep"] == 2 and NSLOW % (128 * group) == 0 and shots % 128 == 0


def body(chips, fused, recorded, receiver_x, source_x):
    per_device = recorded.shape[1]
    first_freq = lax.axis_index("freq") * per_device
    outs = []
    for k in range(per_device):
        omega = two_pi * (base_hertz + step_hertz * (first_freq + k).astype(jnp.float32))
        if fused(recorded.shape[2]):
            first_hertz = functools.partial(lambda k, f: f * per_device + k, k)
            outs.append(one_frequency_fused(chips, first_hertz, recorded[:, k], receiver_x, source_x))
        else:
            outs.append(one_frequency(recorded[:, k], receiver_x, source_x, omega))
    return jnp.stack(outs, axis=1)


def solution(mesh):
    return jax.shard_map(
        functools.partial(body, mesh.shape["shot"], functools.partial(fits, mesh.shape)),
        mesh=mesh,
        in_specs=(P(None, ("parts", "freq"), ("shot", "rep"), None), P("parts"), P("parts")),
        out_specs=P(None, ("parts", "freq"), ("shot", "rep"), None),
        check_vma=False,
    )
```
